32 devices in a mesh: row: 16 (over z, x, core), ch: 2 (over y).
Axes of the slice: x: 2, y: 2, z: 4, core: 2. Of those that a mesh axis runs over, the one named last changes fastest.
Arguments:
- pair_rep: float32 [256, 256, 128], P('row', 'ch'), may hold values from -6 to 6
- residue_mask: int32 [256], replicated, may hold values 0 or 1
- pair_gain: float32 [2, 128], replicated, may hold values from 0.5 to 1.5
- pair_shift: float32 [2, 128], replicated, may hold values from -3 to 3
- panel_weight: bfloat16 [2, 128, 512], replicated, may hold values from -0.5 to 0.5
- panel_bias: float32 [2, 512], replicated, may hold values from -3 to 3
- gate_weight: bfloat16 [2, 128, 128], replicated, may hold values from -0.5 to 0.5
- gate_bias: float32 [2, 128], replicated, may hold values from -3 to 3
- hidden_gain: float32 [2, 128], replicated, may hold values from 0.5 to 1.5
- hidden_shift: float32 [2, 128], replicated, may hold values from -3 to 3
- output_weight: bfloat16 [2, 128, 128], replicated, may hold values from -0.5 to 0.5
- output_bias: float32 [2, 128], replicated, may hold values from -3 to 3
Outputs:
- updated_pair: float32 [256, 256, 128], P('row', 'ch')
The draws below stay inside these ranges and needn't reach their ends.
All inputs are finite; a program needn't handle non-finite values.
Results may differ from the reference program's by a relative error of at most 0.0039.
Values may be sent and summed in bfloat16 or wider, within the bound.
No kernel may reach another device: no remote copies, remote signals or barrier semaphores. Data moves between devices by JAX's collectives and lax.ppermute only.
A program may use at most 64 MiB of HBM per device.

```python
import math
import jax
import jax.numpy as jnp
from jax import lax

C = 128
H = 128
N = 256


def place_ends(array, rng, low, largest):
    spot = [jax.random.randint(jax.random.fold_in(rng, axis), (), 0, length) for axis, length in enumerate(array.shape)]
    widest = array.shape.index(max(array.shape))
    neighbour = spot[:widest] + [(spot[widest] + 1) % array.shape[widest]] + spot[widest + 1:]
    return array.at[tuple(spot)].set(low).at[tuple(neighbour)].set(largest)


def levels(own_key, extent, cuts, smallest, top_value):
    factor_of, own = 1.0, jax.random.fold_in(own_key, 6)
    for axis_at, parts in cuts:
        steps = jnp.exp(jax.random.uniform(jax.random.fold_in(own, axis_at), (parts,), jnp.float32, smallest / len(cuts), top_value / len(cuts)))
        factor_of = factor_of * jnp.repeat(steps, extent[axis_at] // parts).reshape([-1 if axis == axis_at else 1 for axis in range(len(extent))])
    return factor_of


def noise(stream_key, dims, scale, most, cuts=(), kind=jnp.bfloat16):
    array = jax.random.normal(stream_key, dims, jnp.float32) * scale
    if len(cuts) > 0:
        array = levels(stream_key, dims, cuts, -0.22, 0.18) * array
    return jnp.clip(array, min=-most, max=most).astype(kind)


def setup_inputs(seed: int = 0) -> dict:
    key_of = jax.random.split(jax.random.key(seed), 13)
    pair_rep = noise(key_of[0], (N, N, C), 1.0, 6.0, ((0, 16), (1, 2)), jnp.float32)
    residue_mask = place_ends((jax.random.randint(key_of[1], (N,), 0, 8) < 7).astype(jnp.int32), jax.random.fold_in(key_of[1], 1), 0, 1)
    pair_gain = jnp.clip(jax.random.uniform(key_of[2], (2, C), jnp.float32, 0.5, 1.5), 0.5, 1.5)
    pair_shift = noise(key_of[3], (2, C), 0.5, 3.0, (), jnp.float32)
    panel_weight = noise(key_of[4], (2, C, 4 * H), C ** -0.5, 0.5)
    panel_bias = noise(key_of[5], (2, 4 * H), 0.5, 3.0, (), jnp.float32)
    gate_weight = noise(key_of[6], (2, C, C), C ** -0.5, 0.5)
    gate_bias = noise(key_of[7], (2, C), 0.5, 3.0, (), jnp.float32)
    hidden_gain = jnp.clip(jax.random.uniform(key_of[8], (2, H), jnp.float32, 0.5, 1.5), 0.5, 1.5)
    hidden_shift = noise(key_of[9], (2, H), 0.5, 3.0, (), jnp.float32)
    output_weight = noise(key_of[10], (2, H, C), H ** -0.5, 0.5)
    output_bias = noise(key_of[11], (2, C), 0.5, 3.0, (), jnp.float32)
    return dict(pair_rep=pair_rep, residue_mask=residue_mask, pair_gain=pair_gain, pair_shift=pair_shift, panel_weight=panel_weight, panel_bias=panel_bias, gate_weight=gate_weight, gate_bias=gate_bias, hidden_gain=hidden_gain, hidden_shift=hidden_shift, output_weight=output_weight, output_bias=output_bias)


PAIR_EPSILON = 1e-05
HIDDEN_EPSILON = 1.0

def layer_norm(values, gain_value, shift_value, along, epsilon):
    center = lax.optimization_barrier(jnp.mean(values, axis=along, keepdims=True))
    offset = values - center
    spread = lax.optimization_barrier(jnp.mean(offset * offset, axis=along, keepdims=True))
    return offset * lax.rsqrt(spread + epsilon) * gain_value + shift_value

def update(current, cell_mask, section_index, pair_gain, pair_shift, panel_weight, panel_bias, gate_weight, gate_bias, hidden_gain, hidden_shift, output_weight, output_bias):
    normed = layer_norm(current, pair_gain[section_index], pair_shift[section_index], -1, PAIR_EPSILON).astype(jnp.bfloat16)
    flattened = normed.reshape(N * N, C)
    weight = panel_weight[section_index]
    biases = panel_bias[section_index]

    def column(which_one):
        result = jnp.dot(flattened, weight[:, which_one * H:(which_one + 1) * H], preferred_element_type=jnp.float32)
        return (result + biases[which_one * H:(which_one + 1) * H]).reshape(N, N, H)
    left_panel = (cell_mask[:, :, None] * jax.nn.sigmoid(column(0)) * column(1)).astype(jnp.bfloat16)
    right_panel = (cell_mask[:, :, None] * jax.nn.sigmoid(column(2)) * column(3)).astype(jnp.bfloat16)
    gate_value = jax.nn.sigmoid(jnp.dot(flattened, gate_weight[section_index], preferred_element_type=jnp.float32) + gate_bias[section_index]).reshape(N, N, C)
    if section_index == 1:
        left_panel = jnp.transpose(left_panel, (1, 0, 2))
        right_panel = jnp.transpose(right_panel, (1, 0, 2))
    left_hidden = jnp.transpose(left_panel, (2, 0, 1)).astype(jnp.float32)
    right_hidden = jnp.transpose(right_panel, (2, 0, 1)).astype(jnp.float32)
    block_rows = math.gcd(N, 128)
    block_count = N // block_rows
    out_weight = output_weight[section_index].astype(jnp.float32)

    def one_block(block_index):
        row_start = block_index * block_rows
        left_rows = lax.dynamic_slice_in_dim(left_hidden, row_start, block_rows, 1)
        products = jnp.einsum('hik,hjk->hij', left_rows, right_hidden, precision=lax.Precision.HIGHEST)
        normed_hidden = layer_norm(products, hidden_gain[section_index][:, None, None], hidden_shift[section_index][:, None, None], 0, HIDDEN_EPSILON).astype(jnp.bfloat16)
        projected = jnp.einsum('hij,hc->ijc', normed_hidden.astype(jnp.float32), out_weight, precision=lax.Precision.HIGHEST)
        gate_rows = lax.dynamic_slice_in_dim(gate_value, row_start, block_rows, 0)
        return gate_rows * (projected + output_bias[section_index])
    updates = lax.map(one_block, jnp.arange(block_count, dtype=jnp.int32))
    return current + updates.reshape(N, N, C)

def reference(pair_rep, residue_mask, pair_gain, pair_shift, panel_weight, panel_bias, gate_weight, gate_bias, hidden_gain, hidden_shift, output_weight, output_bias):
    residue_float = residue_mask.astype(jnp.float32)
    cell_mask = residue_float[:, None] * residue_float[None, :]
    current = pair_rep
    for section_index in range(2):
        current = update(current, cell_mask, section_index, pair_gain, pair_shift, panel_weight, panel_bias, gate_weight, gate_bias, hidden_gain, hidden_shift, output_weight, output_bias)
    return current
```

```python
import jax
import jax.numpy as jnp
from jax import lax
from jax.sharding import PartitionSpec as P

PAIR_EPSILON = 1e-05
HIDDEN_EPSILON = 1.0


def layer_norm(values, gain_value, shift_value, along, epsilon):
    center = jnp.mean(values, axis=along, keepdims=True)
    offset = values - center
    spread = jnp.mean(offset * offset, axis=along, keepdims=True)
    return offset * lax.rsqrt(spread + epsilon) * gain_value + shift_value


def project(
    current,
    cell_mask,
    section_index,
    pair_gain,
    pair_shift,
    panel_weight,
    panel_bias,
    gate_weight,
    gate_bias,
):
    normed = layer_norm(
        current, pair_gain[section_index], pair_shift[section_index], 2, PAIR_EPSILON
    ).astype(jnp.bfloat16)
    hidden_width = panel_weight.shape[2] // 4
    features = jnp.einsum(
        "rjc,cf->frj", normed, panel_weight[section_index], preferred_element_type=jnp.float32
    )
    features = features + panel_bias[section_index][:, None, None]
    left_panel = (
        cell_mask
        * jax.nn.sigmoid(features[:hidden_width])
        * features[hidden_width : 2 * hidden_width]
    ).astype(jnp.bfloat16)
    right_panel = (
        cell_mask
        * jax.nn.sigmoid(features[2 * hidden_width : 3 * hidden_width])
        * features[3 * hidden_width :]
    ).astype(jnp.bfloat16)
    gate_value = jax.nn.sigmoid(
        jnp.einsum(
            "rjc,cd->rjd", normed, gate_weight[section_index], preferred_element_type=jnp.float32
        )
        + gate_bias[section_index]
    )
    return (left_panel, right_panel, gate_value)


def finish(
    gathered,
    current,
    gate_value,
    section_index,
    hidden_gain,
    hidden_shift,
    output_weight,
    output_bias,
):
    normed = layer_norm(
        gathered,
        hidden_gain[section_index][:, None, None],
        hidden_shift[section_index][:, None, None],
        0,
        HIDDEN_EPSILON,
    ).astype(jnp.bfloat16)
    projected = jnp.einsum(
        "hrj,hc->rjc", normed, output_weight[section_index], preferred_element_type=jnp.float32
    )
    return current + gate_value * (projected + output_bias[section_index])


def local(
    pair_rep,
    residue_mask,
    pair_gain,
    pair_shift,
    panel_weight,
    panel_bias,
    gate_weight,
    gate_bias,
    hidden_gain,
    hidden_shift,
    output_weight,
    output_bias,
):
    row_count = pair_rep.shape[0]
    col_count = pair_rep.shape[1]
    hidden_width = panel_weight.shape[2] // 4
    row_total = lax.axis_size("row")
    col_total = lax.axis_size("ch")
    group = hidden_width // col_total
    if group >= row_total:
        per_slot = group // row_total
        quarters = 1
    else:
        per_slot = 1
        quarters = row_total // group
    slots = row_total // quarters
    sub_rows = row_count // quarters
    blocks = col_count // row_count
    row_index = lax.axis_index("row")
    col_index = lax.axis_index("ch")
    residue_float = residue_mask.astype(jnp.float32)
    row_mask = lax.dynamic_slice_in_dim(residue_float, row_index * row_count, row_count)
    col_mask = lax.dynamic_slice_in_dim(residue_float, col_index * col_count, col_count)
    cell_mask = row_mask[:, None] * col_mask[None, :]
    current = pair_rep
    devices = row_total * col_total
    direct = hidden_width % devices == 0
    for section_index in range(2):
        left_panel, right_panel, gate_value = project(
            current,
            cell_mask,
            section_index,
            pair_gain,
            pair_shift,
            panel_weight,
            panel_bias,
            gate_weight,
            gate_bias,
        )
        if direct:
            own = hidden_width // devices
            send = jnp.concatenate(
                [
                    left_panel.reshape(devices, own, row_count, col_count),
                    right_panel.reshape(devices, own, row_count, col_count),
                ],
                axis=1,
            )
            got = lax.all_to_all(send, ("row", "ch"), split_axis=0, concat_axis=0, tiled=True)
            got = got.reshape(row_total, col_total, 2 * own, row_count, col_count)
            got = jnp.transpose(got, (2, 0, 3, 1, 4)).reshape(
                2 * own, row_total * row_count, col_total * col_count
            )
            pattern = "hik,hjk->hij" if section_index == 0 else "hki,hkj->hij"
            products = jnp.einsum(
                pattern, got[:own], got[own:], preferred_element_type=jnp.float32
            ).astype(jnp.bfloat16)
            returned = products.reshape(own, row_total, row_count, col_total, col_count)
            returned = jnp.transpose(returned, (1, 3, 0, 2, 4)).reshape(
                devices, own, row_count, col_count
            )
            gathered = lax.all_to_all(
                returned, ("row", "ch"), split_axis=0, concat_axis=0, tiled=True
            )
            gathered = gathered.reshape(hidden_width, row_count, col_count).astype(jnp.float32)
            current = finish(
                gathered,
                current,
                gate_value,
                section_index,
                hidden_gain,
                hidden_shift,
                output_weight,
                output_bias,
            )
            continue
        if section_index == 0:
            send_left = left_panel.reshape(
                col_total, slots, per_slot, quarters, sub_rows, col_count
            )
            send_left = jnp.transpose(send_left, (0, 1, 3, 2, 4, 5)).reshape(
                col_total, row_total, per_slot, sub_rows, col_count
            )
        else:
            send_left = left_panel.reshape(
                col_total, slots, per_slot, row_count, blocks, quarters, sub_rows
            )
            send_left = jnp.transpose(send_left, (0, 1, 5, 2, 3, 4, 6)).reshape(
                col_total, row_total, per_slot, row_count, blocks * sub_rows
            )
        send_right = right_panel.reshape(col_total, slots, 1, per_slot, row_count, col_count)
        send_right = jnp.broadcast_to(
            send_right, (col_total, slots, quarters, per_slot, row_count, col_count)
        ).reshape(col_total, row_total, per_slot, row_count, col_count)
        got_left, got_right = (
            lax.all_to_all(
                lax.all_to_all(send_left, "ch", split_axis=0, concat_axis=4, tiled=True),
                "row",
                split_axis=1,
                concat_axis=3,
                tiled=True,
            ),
            lax.all_to_all(
                lax.all_to_all(send_right, "ch", split_axis=0, concat_axis=4, tiled=True),
                "row",
                split_axis=1,
                concat_axis=3,
                tiled=True,
            ),
        )
        got_left = got_left[0, 0]
        got_right = got_right[0, 0]
        if section_index == 0:
            products = jnp.einsum(
                "hik,hjk->hij", got_left, got_right, preferred_element_type=jnp.float32
            )
        else:
            products = jnp.einsum(
                "hki,hkj->hij", got_left, got_right, preferred_element_type=jnp.float32
            )
        returned = products.reshape(per_slot, row_total, sub_rows, col_total, col_count)
        gathered = lax.all_to_all(
            lax.all_to_all(returned, "row", split_axis=1, concat_axis=0, tiled=True),
            "ch",
            split_axis=3,
            concat_axis=0,
            tiled=True,
        )
        gathered = gathered.reshape(col_total, slots, quarters, per_slot, sub_rows, col_count)
        gathered = jnp.transpose(gathered, (0, 1, 3, 2, 4, 5)).reshape(
            hidden_width, row_count, col_count
        )
        current = finish(
            gathered,
            current,
            gate_value,
            section_index,
            hidden_gain,
            hidden_shift,
            output_weight,
            output_bias,
        )
    return current


def solution(mesh):
    return jax.shard_map(
        local,
        mesh=mesh,
        in_specs=(P("row", "ch", None), P(), P(), P(), P(), P(), P(), P(), P(), P(), P(), P()),
        out_specs=P("row", "ch", None),
        check_vma=False,
    )
```

```python
import jax
import jax.numpy as jnp
from jax import lax
from jax.experimental import pallas as pl
from jax.experimental.pallas import tpu as pltpu
from jax.sharding import PartitionSpec as P

PAIR_EPSILON = 1e-05
HIDDEN_EPSILON = 1.0


def layer_norm(values, gain_value, shift_value, along, epsilon):
    center = jnp.mean(values, axis=along, keepdims=True)
    offset = values - center
    spread = jnp.mean(offset * offset, axis=along, keepdims=True)
    return offset * lax.rsqrt(spread + epsilon) * gain_value + shift_value


def project(
    current,
    cell_mask,
    section_index,
    pair_gain,
    pair_shift,
    panel_weight,
    panel_bias,
    gate_weight,
    gate_bias,
):
    normed = layer_norm(
        current, pair_gain[section_index], pair_shift[section_index], 2, PAIR_EPSILON
    ).astype(jnp.bfloat16)
    hidden_width = panel_weight.shape[2] // 4
    features = jnp.einsum(
        "rjc,cf->frj", normed, panel_weight[section_index], preferred_element_type=jnp.float32
    )
    features = features + panel_bias[section_index][:, None, None]
    left_panel = (
        cell_mask
        * jax.nn.sigmoid(features[:hidden_width])
        * features[hidden_width : 2 * hidden_width]
    ).astype(jnp.bfloat16)
    right_panel = (
        cell_mask
        * jax.nn.sigmoid(features[2 * hidden_width : 3 * hidden_width])
        * features[3 * hidden_width :]
    ).astype(jnp.bfloat16)
    gate_value = jax.nn.sigmoid(
        jnp.einsum(
            "rjc,cd->rjd", normed, gate_weight[section_index], preferred_element_type=jnp.float32
        )
        + gate_bias[section_index]
    )
    return (left_panel, right_panel, gate_value)


def finish(
    gathered,
    current,
    gate_value,
    section_index,
    hidden_gain,
    hidden_shift,
    output_weight,
    output_bias,
):
    normed = layer_norm(
        gathered,
        hidden_gain[section_index][:, None, None],
        hidden_shift[section_index][:, None, None],
        0,
        HIDDEN_EPSILON,
    ).astype(jnp.bfloat16)
    projected = jnp.einsum(
        "hrj,hc->rjc", normed, output_weight[section_index], preferred_element_type=jnp.float32
    )
    return current + gate_value * (projected + output_bias[section_index])


def local(
    pair_rep,
    residue_mask,
    pair_gain,
    pair_shift,
    panel_weight,
    panel_bias,
    gate_weight,
    gate_bias,
    hidden_gain,
    hidden_shift,
    output_weight,
    output_bias,
):
    row_count = pair_rep.shape[0]
    col_count = pair_rep.shape[1]
    hidden_width = panel_weight.shape[2] // 4
    row_total = lax.axis_size("row")
    col_total = lax.axis_size("ch")
    group = hidden_width // col_total
    if group >= row_total:
        per_slot = group // row_total
        quarters = 1
    else:
        per_slot = 1
        quarters = row_total // group
    slots = row_total // quarters
    sub_rows = row_count // quarters
    blocks = col_count // row_count
    row_index = lax.axis_index("row")
    col_index = lax.axis_index("ch")
    residue_float = residue_mask.astype(jnp.float32)
    row_mask = lax.dynamic_slice_in_dim(residue_float, row_index * row_count, row_count)
    col_mask = lax.dynamic_slice_in_dim(residue_float, col_index * col_count, col_count)
    cell_mask = row_mask[:, None] * col_mask[None, :]
    current = pair_rep
    for section_index in range(2):
        left_panel, right_panel, gate_value = project(
            current,
            cell_mask,
            section_index,
            pair_gain,
            pair_shift,
            panel_weight,
            panel_bias,
            gate_weight,
            gate_bias,
        )
        if section_index == 0:
            send_left = left_panel.reshape(
                col_total, slots, per_slot, quarters, sub_rows, col_count
            )
            send_left = jnp.transpose(send_left, (0, 1, 3, 2, 4, 5)).reshape(
                col_total, row_total, per_slot, sub_rows, col_count
            )
        else:
            send_left = left_panel.reshape(
                col_total, slots, per_slot, row_count, blocks, quarters, sub_rows
            )
            send_left = jnp.transpose(send_left, (0, 1, 5, 2, 3, 4, 6)).reshape(
                col_total, row_total, per_slot, row_count, blocks * sub_rows
            )
        send_right = right_panel.reshape(col_total, slots, 1, per_slot, row_count, col_count)
        send_right = jnp.broadcast_to(
            send_right, (col_total, slots, quarters, per_slot, row_count, col_count)
        ).reshape(col_total, row_total, per_slot, row_count, col_count)
        got_left, got_right = (
            lax.all_to_all(
                lax.all_to_all(send_left, "ch", split_axis=0, concat_axis=4, tiled=True),
                "row",
                split_axis=1,
                concat_axis=3,
                tiled=True,
            ),
            lax.all_to_all(
                lax.all_to_all(send_right, "ch", split_axis=0, concat_axis=4, tiled=True),
                "row",
                split_axis=1,
                concat_axis=3,
                tiled=True,
            ),
        )
        got_left = got_left[0, 0]
        got_right = got_right[0, 0]
        if section_index == 0:
            products = jnp.einsum(
                "hik,hjk->hij", got_left, got_right, preferred_element_type=jnp.float32
            )
        else:
            products = jnp.einsum(
                "hki,hkj->hij", got_left, got_right, preferred_element_type=jnp.float32
            )
        returned = products.reshape(per_slot, row_total, sub_rows, col_total, col_count)
        gathered = lax.all_to_all(
            lax.all_to_all(returned, "row", split_axis=1, concat_axis=0, tiled=True),
            "ch",
            split_axis=3,
            concat_axis=0,
            tiled=True,
        )
        gathered = gathered.reshape(col_total, slots, quarters, per_slot, sub_rows, col_count)
        gathered = jnp.transpose(gathered, (0, 1, 3, 2, 4, 5)).reshape(
            hidden_width, row_count, col_count
        )
        current = finish(
            gathered,
            current,
            gate_value,
            section_index,
            hidden_gain,
            hidden_shift,
            output_weight,
            output_bias,
        )
    return current


CONTRACT_LAST = (((1,), (1,)), ((), ()))
CONTRACT_FIRST = (((0,), (0,)), ((), ()))


def spread(values, width):
    return jnp.broadcast_to(values, (width, values.shape[1])).T


def cell_row_mask(row_mask_ref, col_mask_ref, row):
    first = lax.axis_index("row") * row_mask_ref.shape[0] // lax.axis_size("row")
    col_mask = col_mask_ref[pl.ds(lax.axis_index("ch"), 1), :].astype(jnp.float32)
    return row_mask_ref[first + row].astype(jnp.float32) * col_mask


def project_setup(section, panel_weight_ref, panel_bias_ref, weight_ref, bias_ref):
    weight_ref[...] = panel_weight_ref[section].astype(jnp.float32).T.astype(jnp.bfloat16)
    bias_ref[...] = spread(panel_bias_ref[section : section + 1, :], bias_ref.shape[1])


def project_row(
    section, row, values, mask, gain_ref, shift_ref, weight_ref, bias_ref, normed_ref, panel_ref
):
    hidden = weight_ref.shape[0] // 4
    normed = layer_norm(
        values,
        gain_ref[section : section + 1, :],
        shift_ref[section : section + 1, :],
        1,
        PAIR_EPSILON,
    ).astype(jnp.bfloat16)
    normed_ref[row] = normed

    def column(which):
        part = pl.ds(which * hidden, hidden)
        return (
            lax.dot_general(
                weight_ref[part, :], normed, CONTRACT_LAST, preferred_element_type=jnp.float32
            )
            + bias_ref[part, :]
        )

    panel_ref[row, :hidden] = mask * jax.nn.sigmoid(column(0)) * column(1)
    panel_ref[row, hidden:] = mask * jax.nn.sigmoid(column(2)) * column(3)


def pack_panels(panel_ref, send_ref):
    own = send_ref.shape[1] // 2
    hidden = panel_ref.shape[1] // 2
    for side in range(2):
        for first in range(0, hidden, 8):
            block = panel_ref[:, side * hidden + first : side * hidden + first + 8, :]
            block = jnp.transpose(block, (1, 0, 2)).astype(jnp.bfloat16)
            for at in range(0, 8, own):
                send_ref[(first + at) // own, side * own : (side + 1) * own] = block[at : at + own]


def open_kernel(
    section,
    row_mask_ref,
    col_mask_ref,
    current_ref,
    gain_ref,
    shift_ref,
    panel_weight_ref,
    panel_bias_ref,
    send_ref,
    normed_ref,
    weight_ref,
    bias_ref,
    panel_ref,
):
    project_setup(section, panel_weight_ref, panel_bias_ref, weight_ref, bias_ref)
    for row in range(current_ref.shape[0]):
        mask = cell_row_mask(row_mask_ref, col_mask_ref, row)
        project_row(
            section,
            row,
            current_ref[row],
            mask,
            gain_ref,
            shift_ref,
            weight_ref,
            bias_ref,
            normed_ref,
            panel_ref,
        )
    pack_panels(panel_ref, send_ref)


def product_kernel(section, got_ref, out_ref):
    rows, cols, both, row_count, col_count = got_ref.shape
    own = both // 2
    total = rows * row_count

    def load(col, index):
        return got_ref[:, col, index].reshape(total, col_count)

    for index in range(own):
        left = [load(col, index) for col in range(cols)]
        right = [load(col, own + index) for col in range(cols)]
        if section == 0:
            products = lax.dot_general(
                jnp.concatenate(left, axis=1),
                jnp.concatenate(right, axis=1),
                CONTRACT_LAST,
                preferred_element_type=jnp.float32,
            )
        else:
            products = lax.dot_general(
                jnp.concatenate(left, axis=1),
                jnp.concatenate(right, axis=1),
                CONTRACT_FIRST,
                preferred_element_type=jnp.float32,
            )
        products = products.astype(jnp.bfloat16)
        for col in range(cols):
            out_ref[:, col, index] = products[:, col * col_count : (col + 1) * col_count].reshape(
                rows, row_count, col_count
            )


def close_rows(
    section,
    gathered_ref,
    current_ref,
    normed_ref,
    gate_weight_ref,
    gate_bias_ref,
    hidden_gain_ref,
    hidden_shift_ref,
    output_weight_ref,
    output_bias_ref,
    turned_ref,
):
    hidden, rows, width = gathered_ref.shape
    values = gathered_ref[...].astype(jnp.float32)
    center = jnp.mean(values, axis=0)
    offset = values - center[None]
    scale = lax.rsqrt(jnp.mean(offset * offset, axis=0) + HIDDEN_EPSILON)
    for first in range(0, hidden, 8):
        block = (gathered_ref[first : first + 8].astype(jnp.float32) - center[None]) * scale[None]
        turned_ref[:, first : first + 8, :] = jnp.transpose(block, (1, 0, 2))
    gain = spread(hidden_gain_ref[section : section + 1, :], width)
    shift = spread(hidden_shift_ref[section : section + 1, :], width)
    for row in range(rows):
        hidden_normed = (turned_ref[row] * gain + shift).astype(jnp.bfloat16)
        projected = lax.dot_general(
            hidden_normed,
            output_weight_ref[section],
            CONTRACT_FIRST,
            preferred_element_type=jnp.float32,
        )
        gate = jax.nn.sigmoid(
            jnp.dot(
                normed_ref[row], gate_weight_ref[section], preferred_element_type=jnp.float32
            )
            + gate_bias_ref[section : section + 1, :]
        )
        yield row, current_ref[row] + gate * (projected + output_bias_ref[section : section + 1, :])


def close_kernel(section, *refs):
    out_ref = refs[9]
    for row, values in close_rows(section, *refs[:9], refs[10]):
        out_ref[row] = values


def middle_kernel(section, *refs):
    row_mask_ref, col_mask_ref, gain_ref, shift_ref, panel_weight_ref, panel_bias_ref = refs[9:15]
    out_ref, send_ref, normed_ref, turned_ref, weight_ref, bias_ref, panel_ref = refs[15:]
    project_setup(section + 1, panel_weight_ref, panel_bias_ref, weight_ref, bias_ref)
    for row, values in close_rows(section, *refs[:9], turned_ref):
        out_ref[row] = values
        project_row(
            section + 1,
            row,
            values,
            cell_row_mask(row_mask_ref, col_mask_ref, row),
            gain_ref,
            shift_ref,
            weight_ref,
            bias_ref,
            normed_ref,
            panel_ref,
        )
    pack_panels(panel_ref, send_ref)


def local_direct(
    pair_rep,
    residue_mask,
    pair_gain,
    pair_shift,
    panel_weight,
    panel_bias,
    gate_weight,
    gate_bias,
    hidden_gain,
    hidden_shift,
    output_weight,
    output_bias,
):
    row_count, col_count, channels = pair_rep.shape
    rows = lax.axis_size("row")
    cols = lax.axis_size("ch")
    devices = rows * cols
    hidden = panel_weight.shape[2] // 4
    own = hidden // devices
    vmem = pl.BlockSpec(memory_space=pltpu.VMEM)
    smem = pl.BlockSpec(memory_space=pltpu.SMEM)
    shape = jax.ShapeDtypeStruct
    send_shape = shape((devices, 2 * own, row_count, col_count), jnp.bfloat16)
    normed_shape = shape((row_count, col_count, channels), jnp.bfloat16)
    pair_shape = shape(pair_rep.shape, jnp.float32)
    project_scratch = [
        pltpu.VMEM((4 * hidden, channels), jnp.bfloat16),
        pltpu.VMEM((4 * hidden, col_count), jnp.float32),
        pltpu.VMEM((row_count, 2 * hidden, col_count), jnp.float32),
    ]
    close_scratch = [pltpu.VMEM((row_count, hidden, col_count), jnp.float32)]
    col_mask = residue_mask.reshape(cols, col_count)

    def exchange(values):
        return lax.all_to_all(values, ("row", "ch"), split_axis=0, concat_axis=0, tiled=True)

    def triangle(section, send):
        got = exchange(send).reshape(rows, cols, 2 * own, row_count, col_count)
        products = pl.pallas_call(
            lambda *refs: product_kernel(section, *refs),
            out_shape=shape((rows, cols, own, row_count, col_count), jnp.bfloat16),
            in_specs=[vmem],
            out_specs=vmem,
            name=f"products_{section}",
        )(got)
        back = exchange(products.reshape(devices, own, row_count, col_count))
        return back.reshape(hidden, row_count, col_count)

    send, normed = pl.pallas_call(
        lambda *refs: open_kernel(0, *refs),
        out_shape=(send_shape, normed_shape),
        in_specs=[smem] + [vmem] * 6,
        out_specs=(vmem, vmem),
        scratch_shapes=project_scratch,
        name="open",
    )(residue_mask, col_mask, pair_rep, pair_gain, pair_shift, panel_weight, panel_bias)
    closing = (gate_weight, gate_bias, hidden_gain, hidden_shift, output_weight, output_bias)
    gathered = triangle(0, send)
    current, send, normed = pl.pallas_call(
        lambda *refs: middle_kernel(0, *refs),
        out_shape=(pair_shape, send_shape, normed_shape),
        in_specs=[vmem] * 9 + [smem] + [vmem] * 5,
        out_specs=(vmem, vmem, vmem),
        scratch_shapes=close_scratch + project_scratch,
        name="middle",
    )(
        gathered,
        pair_rep,
        normed,
        *closing,
        residue_mask,
        col_mask,
        pair_gain,
        pair_shift,
        panel_weight,
        panel_bias,
    )
    gathered = triangle(1, send)
    return pl.pallas_call(
        lambda *refs: close_kernel(1, *refs),
        out_shape=pair_shape,
        in_specs=[vmem] * 9,
        out_specs=vmem,
        scratch_shapes=close_scratch,
        name="close",
    )(gathered, current, normed, *closing)


def solution(mesh):
    devices = mesh.shape["row"] * mesh.shape["ch"]

    def body(*args):
        hidden = args[4].shape[2] // 4
        if hidden % devices == 0 and 8 % (hidden // devices) == 0 and args[0].shape[0] % 16 == 0:
            return local_direct(*args)
        return local(*args)

    return jax.shard_map(
        body,
        mesh=mesh,
        in_specs=(P("row", "ch", None), P(), P(), P(), P(), P(), P(), P(), P(), P(), P(), P()),
        out_specs=P("row", "ch", None),
        check_vma=False,
    )
```

```python
import jax
import jax.numpy as jnp
from jax import lax
from jax.experimental import pallas as pl
from jax.experimental.pallas import tpu as pltpu
from jax.sharding import PartitionSpec as P

PAIR_EPSILON = 1e-05
HIDDEN_EPSILON = 1.0


def layer_norm(values, gain_value, shift_value, along, epsilon):
    center = jnp.mean(values, axis=along, keepdims=True)
    offset = values - center
    spread = jnp.mean(offset * offset, axis=along, keepdims=True)
    return offset * lax.rsqrt(spread + epsilon) * gain_value + shift_value


def project(
    current,
    cell_mask,
    section_index,
    pair_gain,
    pair_shift,
    panel_weight,
    panel_bias,
    gate_weight,
    gate_bias,
):
    normed = layer_norm(
        current, pair_gain[section_index], pair_shift[section_index], 2, PAIR_EPSILON
    ).astype(jnp.bfloat16)
    hidden_width = panel_weight.shape[2] // 4
    features = jnp.einsum(
        "rjc,cf->frj", normed, panel_weight[section_index], preferred_element_type=jnp.float32
    )
    features = features + panel_bias[section_index][:, None, None]
    left_panel = (
        cell_mask
        * jax.nn.sigmoid(features[:hidden_width])
        * features[hidden_width : 2 * hidden_width]
    ).astype(jnp.bfloat16)
    right_panel = (
        cell_mask
        * jax.nn.sigmoid(features[2 * hidden_width : 3 * hidden_width])
        * features[3 * hidden_width :]
    ).astype(jnp.bfloat16)
    gate_value = jax.nn.sigmoid(
        jnp.einsum(
            "rjc,cd->rjd", normed, gate_weight[section_index], preferred_element_type=jnp.float32
        )
        + gate_bias[section_index]
    )
    return (left_panel, right_panel, gate_value)


def finish(
    gathered,
    current,
    gate_value,
    section_index,
    hidden_gain,
    hidden_shift,
    output_weight,
    output_bias,
):
    normed = layer_norm(
        gathered,
        hidden_gain[section_index][:, None, None],
        hidden_shift[section_index][:, None, None],
        0,
        HIDDEN_EPSILON,
    ).astype(jnp.bfloat16)
    projected = jnp.einsum(
        "hrj,hc->rjc", normed, output_weight[section_index], preferred_element_type=jnp.float32
    )
    return current + gate_value * (projected + output_bias[section_index])


def local(
    pair_rep,
    residue_mask,
    pair_gain,
    pair_shift,
    panel_weight,
    panel_bias,
    gate_weight,
    gate_bias,
    hidden_gain,
    hidden_shift,
    output_weight,
    output_bias,
):
    row_count = pair_rep.shape[0]
    col_count = pair_rep.shape[1]
    hidden_width = panel_weight.shape[2] // 4
    row_total = lax.axis_size("row")
    col_total = lax.axis_size("ch")
    group = hidden_width // col_total
    if group >= row_total:
        per_slot = group // row_total
        quarters = 1
    else:
        per_slot = 1
        quarters = row_total // group
    slots = row_total // quarters
    sub_rows = row_count // quarters
    blocks = col_count // row_count
    row_index = lax.axis_index("row")
    col_index = lax.axis_index("ch")
    residue_float = residue_mask.astype(jnp.float32)
    row_mask = lax.dynamic_slice_in_dim(residue_float, row_index * row_count, row_count)
    col_mask = lax.dynamic_slice_in_dim(residue_float, col_index * col_count, col_count)
    cell_mask = row_mask[:, None] * col_mask[None, :]
    current = pair_rep
    for section_index in range(2):
        left_panel, right_panel, gate_value = project(
            current,
            cell_mask,
            section_index,
            pair_gain,
            pair_shift,
            panel_weight,
            panel_bias,
            gate_weight,
            gate_bias,
        )
        if section_index == 0:
            send_left = left_panel.reshape(
                col_total, slots, per_slot, quarters, sub_rows, col_count
            )
            send_left = jnp.transpose(send_left, (0, 1, 3, 2, 4, 5)).reshape(
                col_total, row_total, per_slot, sub_rows, col_count
            )
        else:
            send_left = left_panel.reshape(
                col_total, slots, per_slot, row_count, blocks, quarters, sub_rows
            )
            send_left = jnp.transpose(send_left, (0, 1, 5, 2, 3, 4, 6)).reshape(
                col_total, row_total, per_slot, row_count, blocks * sub_rows
            )
        send_right = right_panel.reshape(col_total, slots, 1, per_slot, row_count, col_count)
        send_right = jnp.broadcast_to(
            send_right, (col_total, slots, quarters, per_slot, row_count, col_count)
        ).reshape(col_total, row_total, per_slot, row_count, col_count)
        got_left, got_right = (
            lax.all_to_all(
                lax.all_to_all(send_left, "ch", split_axis=0, concat_axis=4, tiled=True),
                "row",
                split_axis=1,
                concat_axis=3,
                tiled=True,
            ),
            lax.all_to_all(
                lax.all_to_all(send_right, "ch", split_axis=0, concat_axis=4, tiled=True),
                "row",
                split_axis=1,
                concat_axis=3,
                tiled=True,
            ),
        )
        got_left = got_left[0, 0]
        got_right = got_right[0, 0]
        if section_index == 0:
            products = jnp.einsum(
                "hik,hjk->hij", got_left, got_right, preferred_element_type=jnp.float32
            )
        else:
            products = jnp.einsum(
                "hki,hkj->hij", got_left, got_right, preferred_element_type=jnp.float32
            )
        returned = products.reshape(per_slot, row_total, sub_rows, col_total, col_count)
        gathered = lax.all_to_all(
            lax.all_to_all(returned, "row", split_axis=1, concat_axis=0, tiled=True),
            "ch",
            split_axis=3,
            concat_axis=0,
            tiled=True,
        )
        gathered = gathered.reshape(col_total, slots, quarters, per_slot, sub_rows, col_count)
        gathered = jnp.transpose(gathered, (0, 1, 3, 2, 4, 5)).reshape(
            hidden_width, row_count, col_count
        )
        current = finish(
            gathered,
            current,
            gate_value,
            section_index,
            hidden_gain,
            hidden_shift,
            output_weight,
            output_bias,
        )
    return current


CONTRACT_LAST = (((1,), (1,)), ((), ()))
CONTRACT_FIRST = (((0,), (0,)), ((), ()))


def spread(values, width):
    return jnp.broadcast_to(values, (width, values.shape[1])).T


def cell_row_mask(row_mask_ref, col_mask_ref, row):
    first = lax.axis_index("row") * row_mask_ref.shape[0] // lax.axis_size("row")
    col_mask = col_mask_ref[pl.ds(lax.axis_index("ch"), 1), :].astype(jnp.float32)
    return row_mask_ref[first + row].astype(jnp.float32) * col_mask


def project_setup(section, panel_weight_ref, panel_bias_ref, weight_ref, bias_ref):
    hidden = weight_ref.shape[0] // 4
    for which in range(4):
        part = slice(which * hidden, (which + 1) * hidden)
        factor = 0.5 if which % 2 == 0 else 1.0
        weight = panel_weight_ref[section, :, part].astype(jnp.float32) * factor
        weight_ref[part, :] = weight.T.astype(jnp.bfloat16)
        bias_ref[part, :] = spread(
            panel_bias_ref[section : section + 1, part] * factor, bias_ref.shape[1]
        )


def project_rows(
    section, row, values, masks, gain_ref, shift_ref, weight_ref, bias_ref, normed_ref, panel_ref
):
    hidden = weight_ref.shape[0] // 4
    width = panel_ref.shape[2]
    normed = []
    for at, value in enumerate(values):
        normed.append(
            layer_norm(
                value,
                gain_ref[section : section + 1, :],
                shift_ref[section : section + 1, :],
                1,
                PAIR_EPSILON,
            ).astype(jnp.bfloat16)
        )
        normed_ref[row + at] = normed[at]
    cells = jnp.concatenate(normed, axis=0)

    def column(which):
        return lax.dot_general(
            weight_ref[which * hidden : (which + 1) * hidden, :],
            cells,
            CONTRACT_LAST,
            preferred_element_type=jnp.float32,
        )

    for side in range(2):
        gates = column(2 * side)
        panel = column(2 * side + 1)
        gate_bias = bias_ref[2 * side * hidden : (2 * side + 1) * hidden, :]
        panel_bias = bias_ref[(2 * side + 1) * hidden : (2 * side + 2) * hidden, :]
        for at in range(len(values)):
            lanes = slice(at * width, (at + 1) * width)
            turn = jnp.tanh(gates[:, lanes] + gate_bias)
            half = (0.5 * masks[at]) * (panel[:, lanes] + panel_bias)
            panel_ref[row + at, side * hidden : (side + 1) * hidden] = half + half * turn


def pack_panels(panel_ref, send_ref):
    own = send_ref.shape[1] // 2
    hidden = panel_ref.shape[1] // 2
    for side in range(2):
        for first in range(0, hidden, 8):
            block = panel_ref[:, side * hidden + first : side * hidden + first + 8, :]
            block = jnp.transpose(block, (1, 0, 2)).astype(jnp.bfloat16)
            for at in range(0, 8, own):
                send_ref[(first + at) // own, side * own : (side + 1) * own] = block[at : at + own]


def open_kernel(
    section,
    row_mask_ref,
    col_mask_ref,
    current_ref,
    gain_ref,
    shift_ref,
    panel_weight_ref,
    panel_bias_ref,
    send_ref,
    normed_ref,
    weight_ref,
    bias_ref,
    panel_ref,
):
    project_setup(section, panel_weight_ref, panel_bias_ref, weight_ref, bias_ref)
    for row in range(0, current_ref.shape[0], 2):
        project_rows(
            section,
            row,
            [current_ref[row], current_ref[row + 1]],
            [cell_row_mask(row_mask_ref, col_mask_ref, row + at) for at in range(2)],
            gain_ref,
            shift_ref,
            weight_ref,
            bias_ref,
            normed_ref,
            panel_ref,
        )
    pack_panels(panel_ref, send_ref)


def product_kernel(section, got_ref, out_ref):
    rows, cols, both, row_count, col_count = got_ref.shape
    own = both // 2
    total = rows * row_count

    def load(col, index):
        return got_ref[:, col, index].reshape(total, col_count)

    for index in range(own):
        left = [load(col, index) for col in range(cols)]
        right = [load(col, own + index) for col in range(cols)]
        if section == 0:
            products = lax.dot_general(
                jnp.concatenate(left, axis=1),
                jnp.concatenate(right, axis=1),
                CONTRACT_LAST,
                preferred_element_type=jnp.float32,
            )
        else:
            products = lax.dot_general(
                jnp.concatenate(left, axis=1),
                jnp.concatenate(right, axis=1),
                CONTRACT_FIRST,
                preferred_element_type=jnp.float32,
            )
        products = products.astype(jnp.bfloat16)
        for col in range(cols):
            out_ref[:, col, index] = products[:, col * col_count : (col + 1) * col_count].reshape(
                rows, row_count, col_count
            )


def close_rows(
    section,
    gathered_ref,
    current_ref,
    normed_ref,
    gate_weight_ref,
    gate_bias_ref,
    hidden_gain_ref,
    hidden_shift_ref,
    output_weight_ref,
    output_bias_ref,
    turned_ref,
):
    hidden, rows, width = gathered_ref.shape
    firsts = range(0, hidden, 8)

    def block(first):
        return gathered_ref[first : first + 8].astype(jnp.float32)

    center = sum(jnp.sum(block(first), axis=0) for first in firsts) / hidden
    spread_sum = sum(jnp.sum((block(first) - center[None]) ** 2, axis=0) for first in firsts)
    scale = lax.rsqrt(spread_sum / hidden + HIDDEN_EPSILON)
    for first in firsts:
        turned_ref[:, first : first + 8, :] = jnp.transpose(
            (block(first) - center[None]) * scale[None], (1, 0, 2)
        )
    gain = spread(hidden_gain_ref[section : section + 1, :], width)
    shift = spread(hidden_shift_ref[section : section + 1, :], width)
    output_bias = output_bias_ref[section : section + 1, :]
    gate_weight = (gate_weight_ref[section].astype(jnp.float32) * 0.5).astype(jnp.bfloat16)
    gate_bias = gate_bias_ref[section : section + 1, :] * 0.5
    for row in range(0, rows, 2):
        pair = []
        for at in range(2):
            hidden_normed = (turned_ref[row + at] * gain + shift).astype(jnp.bfloat16)
            projected = lax.dot_general(
                hidden_normed,
                output_weight_ref[section],
                CONTRACT_FIRST,
                preferred_element_type=jnp.float32,
            )
            turn = jnp.tanh(
                jnp.dot(normed_ref[row + at], gate_weight, preferred_element_type=jnp.float32)
                + gate_bias
            )
            half = 0.5 * (projected + output_bias)
            pair.append(current_ref[row + at] + (half + half * turn))
        yield row, pair


def close_kernel(section, *refs):
    out_ref = refs[9]
    for row, values in close_rows(section, *refs[:9], refs[10]):
        out_ref[row] = values[0]
        out_ref[row + 1] = values[1]


def middle_kernel(section, *refs):
    row_mask_ref, col_mask_ref, gain_ref, shift_ref, panel_weight_ref, panel_bias_ref = refs[9:15]
    out_ref, send_ref, normed_ref, turned_ref, weight_ref, bias_ref, panel_ref = refs[15:]
    project_setup(section + 1, panel_weight_ref, panel_bias_ref, weight_ref, bias_ref)
    for row, values in close_rows(section, *refs[:9], turned_ref):
        out_ref[row] = values[0]
        out_ref[row + 1] = values[1]
        project_rows(
            section + 1,
            row,
            values,
            [cell_row_mask(row_mask_ref, col_mask_ref, row + at) for at in range(2)],
            gain_ref,
            shift_ref,
            weight_ref,
            bias_ref,
            normed_ref,
            panel_ref,
        )
    pack_panels(panel_ref, send_ref)


def local_direct(
    pair_rep,
    residue_mask,
    pair_gain,
    pair_shift,
    panel_weight,
    panel_bias,
    gate_weight,
    gate_bias,
    hidden_gain,
    hidden_shift,
    output_weight,
    output_bias,
):
    row_count, col_count, channels = pair_rep.shape
    rows = lax.axis_size("row")
    cols = lax.axis_size("ch")
    devices = rows * cols
    hidden = panel_weight.shape[2] // 4
    own = hidden // devices
    vmem = pl.BlockSpec(memory_space=pltpu.VMEM)
    smem = pl.BlockSpec(memory_space=pltpu.SMEM)
    shape = jax.ShapeDtypeStruct
    send_shape = shape((devices, 2 * own, row_count, col_count), jnp.bfloat16)
    normed_shape = shape((row_count, col_count, channels), jnp.bfloat16)
    pair_shape = shape(pair_rep.shape, jnp.float32)
    project_scratch = [
        pltpu.VMEM((4 * hidden, channels), jnp.bfloat16),
        pltpu.VMEM((4 * hidden, col_count), jnp.float32),
        pltpu.VMEM((row_count, 2 * hidden, col_count), jnp.float32),
    ]
    close_scratch = [pltpu.VMEM((row_count, hidden, col_count), jnp.float32)]
    col_mask = residue_mask.reshape(cols, col_count)

    def exchange(values):
        return lax.all_to_all(values, ("row", "ch"), split_axis=0, concat_axis=0, tiled=True)

    def triangle(section, send):
        got = exchange(send).reshape(rows, cols, 2 * own, row_count, col_count)
        products = pl.pallas_call(
            lambda *refs: product_kernel(section, *refs),
            out_shape=shape((rows, cols, own, row_count, col_count), jnp.bfloat16),
            in_specs=[vmem],
            out_specs=vmem,
            name=f"products_{section}",
        )(got)
        back = exchange(products.reshape(devices, own, row_count, col_count))
        return back.reshape(hidden, row_count, col_count)

    send, normed = pl.pallas_call(
        lambda *refs: open_kernel(0, *refs),
        out_shape=(send_shape, normed_shape),
        in_specs=[smem] + [vmem] * 6,
        out_specs=(vmem, vmem),
        scratch_shapes=project_scratch,
        name="open",
    )(residue_mask, col_mask, pair_rep, pair_gain, pair_shift, panel_weight, panel_bias)
    closing = (gate_weight, gate_bias, hidden_gain, hidden_shift, output_weight, output_bias)
    gathered = triangle(0, send)
    current, send, normed = pl.pallas_call(
        lambda *refs: middle_kernel(0, *refs),
        out_shape=(pair_shape, send_shape, normed_shape),
        in_specs=[vmem] * 9 + [smem] + [vmem] * 5,
        out_specs=(vmem, vmem, vmem),
        scratch_shapes=close_scratch + project_scratch,
        name="middle",
    )(
        gathered,
        pair_rep,
        normed,
        *closing,
        residue_mask,
        col_mask,
        pair_gain,
        pair_shift,
        panel_weight,
        panel_bias,
    )
    gathered = triangle(1, send)
    return pl.pallas_call(
        lambda *refs: close_kernel(1, *refs),
        out_shape=pair_shape,
        in_specs=[vmem] * 9,
        out_specs=vmem,
        scratch_shapes=close_scratch,
        name="close",
    )(gathered, current, normed, *closing)


def solution(mesh):
    devices = mesh.shape["row"] * mesh.shape["ch"]

    def body(*args):
        hidden = args[4].shape[2] // 4
        if hidden % devices == 0 and 8 % (hidden // devices) == 0 and args[0].shape[0] % 16 == 0:
            return local_direct(*args)
        return local(*args)

    return jax.shard_map(
        body,
        mesh=mesh,
        in_specs=(P("row", "ch", None), P(), P(), P(), P(), P(), P(), P(), P(), P(), P(), P()),
        out_specs=P("row", "ch", None),
        check_vma=False,
    )
```

```python
import jax
import jax.numpy as jnp
from jax import lax
from jax.experimental import pallas as pl
from jax.experimental.pallas import tpu as pltpu
from jax.sharding import PartitionSpec as P

PAIR_EPSILON = 1e-05
HIDDEN_EPSILON = 1.0
GRANT = 32 * 1024 * 1024


def layer_norm(values, gain_value, shift_value, along, epsilon):
    center = jnp.mean(values, axis=along, keepdims=True)
    offset = values - center
    spread = jnp.mean(offset * offset, axis=along, keepdims=True)
    return offset * lax.rsqrt(spread + epsilon) * gain_value + shift_value


def project(
    current,
    cell_mask,
    section_index,
    pair_gain,
    pair_shift,
    panel_weight,
    panel_bias,
    gate_weight,
    gate_bias,
):
    normed = layer_norm(
        current, pair_gain[section_index], pair_shift[section_index], 2, PAIR_EPSILON
    ).astype(jnp.bfloat16)
    hidden_width = panel_weight.shape[2] // 4
    features = jnp.einsum(
        "rjc,cf->frj", normed, panel_weight[section_index], preferred_element_type=jnp.float32
    )
    features = features + panel_bias[section_index][:, None, None]
    left_panel = (
        cell_mask
        * jax.nn.sigmoid(features[:hidden_width])
        * features[hidden_width : 2 * hidden_width]
    ).astype(jnp.bfloat16)
    right_panel = (
        cell_mask
        * jax.nn.sigmoid(features[2 * hidden_width : 3 * hidden_width])
        * features[3 * hidden_width :]
    ).astype(jnp.bfloat16)
    gate_value = jax.nn.sigmoid(
        jnp.einsum(
            "rjc,cd->rjd", normed, gate_weight[section_index], preferred_element_type=jnp.float32
        )
        + gate_bias[section_index]
    )
    return (left_panel, right_panel, gate_value)


def finish(
    gathered,
    current,
    gate_value,
    section_index,
    hidden_gain,
    hidden_shift,
    output_weight,
    output_bias,
):
    normed = layer_norm(
        gathered,
        hidden_gain[section_index][:, None, None],
        hidden_shift[section_index][:, None, None],
        0,
        HIDDEN_EPSILON,
    ).astype(jnp.bfloat16)
    projected = jnp.einsum(
        "hrj,hc->rjc", normed, output_weight[section_index], preferred_element_type=jnp.float32
    )
    return current + gate_value * (projected + output_bias[section_index])


def local(
    pair_rep,
    residue_mask,
    pair_gain,
    pair_shift,
    panel_weight,
    panel_bias,
    gate_weight,
    gate_bias,
    hidden_gain,
    hidden_shift,
    output_weight,
    output_bias,
):
    row_count = pair_rep.shape[0]
    col_count = pair_rep.shape[1]
    hidden_width = panel_weight.shape[2] // 4
    row_total = lax.axis_size("row")
    col_total = lax.axis_size("ch")
    group = hidden_width // col_total
    if group >= row_total:
        per_slot = group // row_total
        quarters = 1
    else:
        per_slot = 1
        quarters = row_total // group
    slots = row_total // quarters
    sub_rows = row_count // quarters
    blocks = col_count // row_count
    row_index = lax.axis_index("row")
    col_index = lax.axis_index("ch")
    residue_float = residue_mask.astype(jnp.float32)
    row_mask = lax.dynamic_slice_in_dim(residue_float, row_index * row_count, row_count)
    col_mask = lax.dynamic_slice_in_dim(residue_float, col_index * col_count, col_count)
    cell_mask = row_mask[:, None] * col_mask[None, :]
    current = pair_rep
    for section_index in range(2):
        left_panel, right_panel, gate_value = project(
            current,
            cell_mask,
            section_index,
            pair_gain,
            pair_shift,
            panel_weight,
            panel_bias,
            gate_weight,
            gate_bias,
        )
        if section_index == 0:
            send_left = left_panel.reshape(
                col_total, slots, per_slot, quarters, sub_rows, col_count
            )
            send_left = jnp.transpose(send_left, (0, 1, 3, 2, 4, 5)).reshape(
                col_total, row_total, per_slot, sub_rows, col_count
            )
        else:
            send_left = left_panel.reshape(
                col_total, slots, per_slot, row_count, blocks, quarters, sub_rows
            )
            send_left = jnp.transpose(send_left, (0, 1, 5, 2, 3, 4, 6)).reshape(
                col_total, row_total, per_slot, row_count, blocks * sub_rows
            )
        send_right = right_panel.reshape(col_total, slots, 1, per_slot, row_count, col_count)
        send_right = jnp.broadcast_to(
            send_right, (col_total, slots, quarters, per_slot, row_count, col_count)
        ).reshape(col_total, row_total, per_slot, row_count, col_count)
        got_left, got_right = (
            lax.all_to_all(
                lax.all_to_all(send_left, "ch", split_axis=0, concat_axis=4, tiled=True),
                "row",
                split_axis=1,
                concat_axis=3,
                tiled=True,
            ),
            lax.all_to_all(
                lax.all_to_all(send_right, "ch", split_axis=0, concat_axis=4, tiled=True),
                "row",
                split_axis=1,
                concat_axis=3,
                tiled=True,
            ),
        )
        got_left = got_left[0, 0]
        got_right = got_right[0, 0]
        if section_index == 0:
            products = jnp.einsum(
                "hik,hjk->hij", got_left, got_right, preferred_element_type=jnp.float32
            )
        else:
            products = jnp.einsum(
                "hki,hkj->hij", got_left, got_right, preferred_element_type=jnp.float32
            )
        returned = products.reshape(per_slot, row_total, sub_rows, col_total, col_count)
        gathered = lax.all_to_all(
            lax.all_to_all(returned, "row", split_axis=1, concat_axis=0, tiled=True),
            "ch",
            split_axis=3,
            concat_axis=0,
            tiled=True,
        )
        gathered = gathered.reshape(col_total, slots, quarters, per_slot, sub_rows, col_count)
        gathered = jnp.transpose(gathered, (0, 1, 3, 2, 4, 5)).reshape(
            hidden_width, row_count, col_count
        )
        current = finish(
            gathered,
            current,
            gate_value,
            section_index,
            hidden_gain,
            hidden_shift,
            output_weight,
            output_bias,
        )
    return current


CONTRACT_LAST = (((1,), (1,)), ((), ()))
CONTRACT_FIRST = (((0,), (0,)), ((), ()))


def spread(values, width):
    return jnp.broadcast_to(values, (width, values.shape[1])).T


def cell_row_mask(row_mask_ref, col_mask_ref, row):
    first = lax.axis_index("row") * row_mask_ref.shape[0] // lax.axis_size("row")
    col_mask = col_mask_ref[pl.ds(lax.axis_index("ch"), 1), :].astype(jnp.float32)
    return row_mask_ref[first + row].astype(jnp.float32) * col_mask


def project_setup(section, panel_weight_ref, panel_bias_ref, weight_ref, bias_ref):
    hidden = weight_ref.shape[0] // 4
    for which in range(4):
        part = slice(which * hidden, (which + 1) * hidden)
        factor = 0.5 if which % 2 == 0 else 1.0
        weight = panel_weight_ref[section, :, part].astype(jnp.float32) * factor
        weight_ref[part, :] = weight.T.astype(jnp.bfloat16)
        bias_ref[part, :] = spread(
            panel_bias_ref[section : section + 1, part] * factor, bias_ref.shape[1]
        )


def project_rows(
    section, row, values, masks, gain_ref, shift_ref, weight_ref, bias_ref, normed_ref, panel_ref
):
    hidden = weight_ref.shape[0] // 4
    width = panel_ref.shape[2]
    normed = []
    for at, value in enumerate(values):
        normed.append(
            layer_norm(
                value,
                gain_ref[section : section + 1, :],
                shift_ref[section : section + 1, :],
                1,
                PAIR_EPSILON,
            ).astype(jnp.bfloat16)
        )
        normed_ref[row + at] = normed[at]
    cells = jnp.concatenate(normed, axis=0)

    def column(which):
        return lax.dot_general(
            weight_ref[which * hidden : (which + 1) * hidden, :],
            cells,
            CONTRACT_LAST,
            preferred_element_type=jnp.float32,
        )

    for side in range(2):
        gates = column(2 * side)
        panel = column(2 * side + 1)
        gate_bias = bias_ref[2 * side * hidden : (2 * side + 1) * hidden, :]
        panel_bias = bias_ref[(2 * side + 1) * hidden : (2 * side + 2) * hidden, :]
        for at in range(len(values)):
            lanes = slice(at * width, (at + 1) * width)
            turn = jnp.tanh(gates[:, lanes] + gate_bias)
            half = (0.5 * masks[at]) * (panel[:, lanes] + panel_bias)
            panel_ref[row + at, side * hidden : (side + 1) * hidden] = half + half * turn


def pack_panels(panel_ref, send_ref):
    own = send_ref.shape[1] // 2
    hidden = panel_ref.shape[1] // 2
    for side in range(2):
        for first in range(0, hidden, 8):
            block = panel_ref[:, side * hidden + first : side * hidden + first + 8, :]
            block = jnp.transpose(block, (1, 0, 2)).astype(jnp.bfloat16)
            for at in range(0, 8, own):
                send_ref[(first + at) // own, side * own : (side + 1) * own] = block[at : at + own]


def open_kernel(
    section,
    row_mask_ref,
    col_mask_ref,
    current_ref,
    gain_ref,
    shift_ref,
    panel_weight_ref,
    panel_bias_ref,
    send_ref,
    normed_ref,
    weight_ref,
    bias_ref,
    panel_ref,
):
    project_setup(section, panel_weight_ref, panel_bias_ref, weight_ref, bias_ref)
    for row in range(0, current_ref.shape[0], 2):
        project_rows(
            section,
            row,
            [current_ref[row], current_ref[row + 1]],
            [cell_row_mask(row_mask_ref, col_mask_ref, row + at) for at in range(2)],
            gain_ref,
            shift_ref,
            weight_ref,
            bias_ref,
            normed_ref,
            panel_ref,
        )
    pack_panels(panel_ref, send_ref)


def product_kernel(section, got_ref, out_ref):
    rows, cols, both, row_count, col_count = got_ref.shape
    own = both // 2
    total = rows * row_count

    def load(col, index):
        return got_ref[:, col, index].reshape(total, col_count)

    for index in range(own):
        left = [load(col, index) for col in range(cols)]
        right = [load(col, own + index) for col in range(cols)]
        if section == 0:
            products = lax.dot_general(
                jnp.concatenate(left, axis=1),
                jnp.concatenate(right, axis=1),
                CONTRACT_LAST,
                preferred_element_type=jnp.float32,
            )
        else:
            products = lax.dot_general(
                jnp.concatenate(left, axis=1),
                jnp.concatenate(right, axis=1),
                CONTRACT_FIRST,
                preferred_element_type=jnp.float32,
            )
        products = products.astype(jnp.bfloat16)
        for col in range(cols):
            out_ref[:, col, index] = products[:, col * col_count : (col + 1) * col_count].reshape(
                rows, row_count, col_count
            )


def close_rows(
    section,
    gathered_ref,
    current_ref,
    normed_ref,
    gate_weight_ref,
    gate_bias_ref,
    hidden_gain_ref,
    hidden_shift_ref,
    output_weight_ref,
    output_bias_ref,
    turned_ref,
):
    hidden, rows, width = gathered_ref.shape
    firsts = range(0, hidden, 8)

    def block(first):
        return gathered_ref[first : first + 8].astype(jnp.float32)

    center = sum(jnp.sum(block(first), axis=0) for first in firsts) / hidden
    spread_sum = sum(jnp.sum((block(first) - center[None]) ** 2, axis=0) for first in firsts)
    scale = lax.rsqrt(spread_sum / hidden + HIDDEN_EPSILON)
    for first in firsts:
        turned_ref[:, first : first + 8, :] = jnp.transpose(
            (block(first) - center[None]) * scale[None], (1, 0, 2)
        )
    gain = spread(hidden_gain_ref[section : section + 1, :], width)
    shift = spread(hidden_shift_ref[section : section + 1, :], width)
    output_bias = output_bias_ref[section : section + 1, :]
    gate_weight = (gate_weight_ref[section].astype(jnp.float32) * 0.5).astype(jnp.bfloat16)
    gate_bias = gate_bias_ref[section : section + 1, :] * 0.5
    for row in range(0, rows, 2):
        pair = []
        for at in range(2):
            hidden_normed = (turned_ref[row + at] * gain + shift).astype(jnp.bfloat16)
            projected = lax.dot_general(
                hidden_normed,
                output_weight_ref[section],
                CONTRACT_FIRST,
                preferred_element_type=jnp.float32,
            )
            turn = jnp.tanh(
                jnp.dot(normed_ref[row + at], gate_weight, preferred_element_type=jnp.float32)
                + gate_bias
            )
            half = 0.5 * (projected + output_bias)
            pair.append(current_ref[row + at] + (half + half * turn))
        yield row, pair


def close_kernel(section, *refs):
    out_ref = refs[9]
    for row, values in close_rows(section, *refs[:9], refs[10]):
        out_ref[row] = values[0]
        out_ref[row + 1] = values[1]


def middle_kernel(section, *refs):
    row_mask_ref, col_mask_ref, gain_ref, shift_ref, panel_weight_ref, panel_bias_ref = refs[9:15]
    out_ref, send_ref, normed_ref, turned_ref, weight_ref, bias_ref, panel_ref = refs[15:]
    project_setup(section + 1, panel_weight_ref, panel_bias_ref, weight_ref, bias_ref)
    for row, values in close_rows(section, *refs[:9], turned_ref):
        out_ref[row] = values[0]
        out_ref[row + 1] = values[1]
        project_rows(
            section + 1,
            row,
            values,
            [cell_row_mask(row_mask_ref, col_mask_ref, row + at) for at in range(2)],
            gain_ref,
            shift_ref,
            weight_ref,
            bias_ref,
            normed_ref,
            panel_ref,
        )
    pack_panels(panel_ref, send_ref)


def local_direct(
    pair_rep,
    residue_mask,
    pair_gain,
    pair_shift,
    panel_weight,
    panel_bias,
    gate_weight,
    gate_bias,
    hidden_gain,
    hidden_shift,
    output_weight,
    output_bias,
):
    row_count, col_count, channels = pair_rep.shape
    rows = lax.axis_size("row")
    cols = lax.axis_size("ch")
    devices = rows * cols
    hidden = panel_weight.shape[2] // 4
    own = hidden // devices
    vmem = pl.BlockSpec(memory_space=pltpu.VMEM)
    smem = pl.BlockSpec(memory_space=pltpu.SMEM)
    shape = jax.ShapeDtypeStruct
    send_shape = pltpu.VMEM((devices, 2 * own, row_count, col_count), jnp.bfloat16)
    pair_shape = shape(pair_rep.shape, jnp.float32)
    normed_kept = pltpu.VMEM((row_count, col_count, channels), jnp.bfloat16)
    pair_kept = pltpu.VMEM(pair_rep.shape, jnp.float32)
    project_scratch = [
        pltpu.VMEM((4 * hidden, channels), jnp.bfloat16),
        pltpu.VMEM((4 * hidden, col_count), jnp.float32),
        pltpu.VMEM((row_count, 2 * hidden, col_count), jnp.float32),
    ]
    close_scratch = [pltpu.VMEM((row_count, hidden, col_count), jnp.float32)]
    col_mask = residue_mask.reshape(cols, col_count)

    def exchange(values):
        return lax.all_to_all(values, ("row", "ch"), split_axis=0, concat_axis=0, tiled=True)

    def triangle(section, send):
        got = exchange(send).reshape(rows, cols, 2 * own, row_count, col_count)
        got = pltpu.with_memory_space_constraint(got, pltpu.VMEM)
        products = pl.pallas_call(
            lambda *refs: product_kernel(section, *refs),
            out_shape=pltpu.VMEM((rows, cols, own, row_count, col_count), jnp.bfloat16),
            in_specs=[vmem],
            out_specs=vmem,
            compiler_params=pltpu.CompilerParams(vmem_limit_bytes=GRANT),
            name=f"products_{section}",
        )(got)
        back = exchange(products.reshape(devices, own, row_count, col_count))
        back = back.reshape(hidden, row_count, col_count)
        return pltpu.with_memory_space_constraint(back, pltpu.VMEM)

    send, normed = pl.pallas_call(
        lambda *refs: open_kernel(0, *refs),
        out_shape=(send_shape, normed_kept),
        in_specs=[smem] + [vmem] * 6,
        out_specs=(vmem, vmem),
        scratch_shapes=project_scratch,
        compiler_params=pltpu.CompilerParams(vmem_limit_bytes=GRANT),
        name="open",
    )(
        residue_mask,
        *(
            pltpu.with_memory_space_constraint(values, pltpu.HBM)
            for values in (col_mask, pair_rep, pair_gain, pair_shift, panel_weight, panel_bias)
        ),
    )
    def keep(values):
        return pltpu.with_memory_space_constraint(values, pltpu.VMEM)

    closing = (gate_weight, gate_bias, hidden_gain, hidden_shift, output_weight, output_bias)
    closing = tuple(keep(values) for values in closing)
    gathered = triangle(0, send)
    current, send, normed = pl.pallas_call(
        lambda *refs: middle_kernel(0, *refs),
        out_shape=(pair_kept, send_shape, normed_kept),
        in_specs=[vmem] * 9 + [smem] + [vmem] * 5,
        out_specs=(vmem, vmem, vmem),
        scratch_shapes=close_scratch + project_scratch,
        compiler_params=pltpu.CompilerParams(vmem_limit_bytes=GRANT),
        name="middle",
    )(
        gathered,
        keep(pair_rep),
        keep(normed),
        *closing,
        residue_mask,
        col_mask,
        pair_gain,
        pair_shift,
        keep(panel_weight),
        panel_bias,
    )
    gathered = triangle(1, send)
    return pl.pallas_call(
        lambda *refs: close_kernel(1, *refs),
        out_shape=pair_shape,
        in_specs=[vmem] * 9,
        out_specs=vmem,
        scratch_shapes=close_scratch,
        compiler_params=pltpu.CompilerParams(vmem_limit_bytes=GRANT),
        name="close",
    )(gathered, keep(current), keep(normed), *closing)


def solution(mesh):
    devices = mesh.shape["row"] * mesh.shape["ch"]

    def body(*args):
        hidden = args[4].shape[2] // 4
        if hidden % devices == 0 and 8 % (hidden // devices) == 0 and args[0].shape[0] % 16 == 0:
            return local_direct(*args)
        return local(*args)

    return jax.shard_map(
        body,
        mesh=mesh,
        in_specs=(P("row", "ch", None), P(), P(), P(), P(), P(), P(), P(), P(), P(), P(), P()),
        out_specs=P("row", "ch", None),
        check_vma=False,
    )
```
